256 devices in a mesh: fsdp: 32 (over x_hi, z, core), tp: 8 (over x_lo, y).
Axes of the slice: x: 4 (x_hi: 2, x_lo: 2; x = x_hi * 2 + x_lo), y: 4, z: 8, core: 2. Of those that a mesh axis runs over, the one named last changes fastest.
Arguments:
- tokens: bfloat16 [4096, 3584], P('fsdp', 'tp'), may hold values from -6 to 6
- norm_gain: bfloat16 [3584], replicated, may hold values from 0.5 to 1.5
- gate_weight: bfloat16 [3584, 10240], P('fsdp', 'tp'), may hold values from -0.09375 to 0.09375
- up_weight: bfloat16 [3584, 10240], P('fsdp', 'tp'), may hold values from -0.09375 to 0.09375
- down_weight: bfloat16 [3584, 10240], P('fsdp', 'tp'), may hold values from -0.0625 to 0.0625
- probes: bfloat16 [2, 3584, 10240], P(None, 'fsdp', 'tp'), may hold values from -0.0625 to 0.0625
Outputs:
- layer_out: bfloat16 [4096, 3584], P('tp', 'fsdp')
- token_curv: float32 [4096], P('tp')
The draws below stay inside these ranges and needn't reach their ends.
All inputs are finite; a program needn't handle non-finite values.
Results may differ from the reference program's by a relative error of at most 0.014.
Values may be sent and summed in bfloat16 or wider, within the bound.
No kernel may reach another device: no remote copies, remote signals or barrier semaphores. Data moves between devices by JAX's collectives and lax.ppermute only.
A program may use at most 64 MiB of HBM per device.

```python
import jax
import jax.numpy as jnp
from jax import lax

D = 3584
FF = 10240
PROBES = 2
TOKENS = 4096
N_TP = 8


def level_of(rng, dims, cuts, smallest, largest):
    def one(dim, parts):
        steps = jax.random.uniform(jax.random.fold_in(jax.random.fold_in(rng, 6), dim), (parts,), jnp.float32, smallest / len(cuts), largest / len(cuts))
        return jnp.repeat(jnp.exp(steps), dims[dim] // parts).reshape((-1,) + (1,) * (len(dims) - dim - 1))

    gain = one(*cuts[0])
    for cut in cuts[1:]:
        gain = gain * one(*cut)
    return gain


def bell_draw(own_key, dims, width, most, shards=(), dtype=jnp.bfloat16):
    factor_of = level_of(own_key, dims, shards, -0.22, 0.18) if shards else 1.0
    entries = jax.random.normal(own_key, dims, jnp.float32) * width * factor_of
    return jnp.minimum(jnp.maximum(entries, -most), most).astype(dtype)


def setup_inputs(seed: int = 0) -> dict:
    arg_keys = jax.random.split(jax.random.key(seed), 7)
    return {
        "tokens": bell_draw(arg_keys[0], (TOKENS, D), 1.0, 6.0, ((0, 32), (1, 8))),
        "norm_gain": jnp.clip(1.0 + 0.1 * jax.random.normal(arg_keys[1], (D,), jnp.float32), 0.5, 1.5).astype(jnp.bfloat16),
        "gate_weight": bell_draw(arg_keys[2], (D, FF), D ** -0.5, 0.09375, ((0, 32), (1, 8))),
        "up_weight": bell_draw(arg_keys[3], (D, FF), D ** -0.5, 0.09375, ((0, 32), (1, 8))),
        "down_weight": bell_draw(arg_keys[4], (D, FF), FF ** -0.5, 0.0625, ((0, 32), (1, 8))),
        "probes": bell_draw(arg_keys[5], (PROBES, D, FF), FF ** -0.5, 0.0625, ((1, 32), (2, 8))),
    }


epsilon = 1e-06

def reference(tokens, norm_gain, gate_weight, up_weight, down_weight, probes):
    widened = tokens.astype(jnp.float32)
    inverse_rms = lax.rsqrt(lax.optimization_barrier(jnp.mean(widened * widened, axis=1, keepdims=True)) + epsilon)
    normed = (widened * inverse_rms * norm_gain.astype(jnp.float32)).astype(jnp.bfloat16)
    gate_sum = jnp.dot(normed, gate_weight, preferred_element_type=jnp.float32)
    up_sum = jnp.dot(normed, up_weight, preferred_element_type=jnp.float32)
    hidden = (jax.nn.silu(gate_sum) * up_sum).astype(jnp.bfloat16)
    stacked = jnp.concatenate([down_weight[None], probes], axis=0)
    count = stacked.shape[0]
    block_width = FF // N_TP

    def add_block(block_index, running):
        offset = (block_index * block_width).astype(jnp.int32)
        columns = lax.dynamic_slice_in_dim(hidden, offset, block_width, 1)
        matrices = lax.dynamic_slice_in_dim(stacked, offset, block_width, 2)
        terms = [lax.dot_general(columns, matrices[which], (((1,), (1,)), ((), ())), preferred_element_type=jnp.float32).astype(jnp.bfloat16).astype(jnp.float32) for which in range(count)]
        return running + jnp.stack(terms)
    projected = lax.fori_loop(0, N_TP, add_block, jnp.zeros((count, TOKENS, D), jnp.float32))
    primal = projected[0]
    squashed = jax.nn.sigmoid(primal)
    slope = squashed * (1.0 - squashed)
    tangent_sq = lax.optimization_barrier(jnp.sum(projected[1:] * projected[1:], axis=0))
    token_curv = lax.optimization_barrier(jnp.sum(slope * tangent_sq, axis=1)) / (PROBES * D)
    return (primal.astype(jnp.bfloat16), token_curv)
```

```python
import jax
import jax.numpy as jnp
from jax import lax
from jax.sharding import Mesh
from jax.sharding import PartitionSpec as P

D = 3584
PROBES = 2
AXES = {"xh": 2, "z": 8, "c": 2, "xl": 2, "y": 4}

epsilon = 1e-06


def moved(array, axes, shift):
    n = lax.axis_size(axes)
    return lax.ppermute(array, axes, [(i, (i + shift) % n) for i in range(n)])


def in_order_of(axis, own, other):
    first = lax.axis_index(axis) == 0
    return jnp.stack([jnp.where(first, own, other), jnp.where(first, other, own)])


def on_device(tokens, norm_gain, gate_weight, up_weight, down_weight, probes):
    rows, units = gate_weight.shape
    part = units // 4

    halves = [w.reshape(rows, 4, part).transpose(1, 0, 2) for w in (gate_weight, up_weight)]
    sent = jnp.concatenate(halves, axis=2)
    got = lax.all_to_all(sent, ("xh", "c"), 0, 0, tiled=True)
    gathered = lax.all_gather(got, "z", axis=0)
    weights = gathered.reshape(8, 2, 2, rows, 2 * part).transpose(1, 0, 2, 3, 4)
    weights = weights.reshape(D, 2 * part)

    block, width = tokens.shape
    spread = jnp.broadcast_to(tokens[None], (8, block, width))
    features = lax.all_to_all(spread, ("xl", "y"), 0, 0, tiled=True)
    features = jnp.moveaxis(features, 0, 1).reshape(block, D)
    widened = features.astype(jnp.float32)
    inverse_rms = lax.rsqrt(jnp.mean(widened * widened, axis=1, keepdims=True) + epsilon)
    own = (widened * inverse_rms * norm_gain.astype(jnp.float32)).astype(jnp.bfloat16)
    pair = in_order_of("xh", own, moved(own, "xh", 1))
    quad = in_order_of("c", pair, moved(pair, "c", 1))
    normed = quad.transpose(1, 0, 2, 3).reshape(4 * block, D)

    sums = jnp.dot(normed, weights, preferred_element_type=jnp.float32)
    gate_sum, up_sum = sums[:, :part], sums[:, part:]
    hidden = (jax.nn.silu(gate_sum) * up_sum).astype(jnp.bfloat16)

    stacked = jnp.concatenate([down_weight[None], probes], axis=0)
    count = stacked.shape[0]
    flat = stacked.reshape(count * rows, units)
    xs = ("xh", "xl")
    ring = [flat] + [moved(flat, xs, s) for s in (1, 2, 3)]
    x = lax.axis_index("xh") * 2 + lax.axis_index("xl")
    ring = jnp.stack(ring)
    by_x = jnp.stack([ring[(x - i) % 4] for i in range(4)])
    by_c = in_order_of("c", by_x, moved(by_x, "c", 1))
    matrices = by_c.reshape(2, 2, 2, count * rows, units).transpose(1, 0, 3, 2, 4)
    matrices = matrices.reshape(4 * count * rows, 2 * units)

    chunks = hidden.reshape(2, 2, 2, block // 2, part).transpose(1, 0, 2, 3, 4)
    chunks = chunks.reshape(8, block // 2, part)
    mine = lax.all_to_all(chunks, ("xh", "xl", "c"), 0, 0, tiled=True)
    mine = mine.reshape(2, 2, 2, block // 2, part).transpose(3, 1, 0, 2, 4)
    mine = mine.reshape(block // 2, 2 * units)
    everyone = lax.all_gather(mine, "z", axis=0, tiled=True)

    terms = lax.dot_general(
        everyone, matrices, (((1,), (1,)), ((), ())), preferred_element_type=jnp.float32
    ).astype(jnp.bfloat16)
    terms = terms.reshape(4, block, 4 * count * rows)
    arrived = lax.all_to_all(terms, "y", 0, 0, tiled=True)
    summed = jnp.sum(arrived.astype(jnp.float32), axis=0)
    summed = summed.reshape(block, 4, count, rows)
    primal = summed[:, :, 0]
    tangents = summed[:, :, 1:]
    squashed = jax.nn.sigmoid(primal)
    slope = squashed * (1.0 - squashed)
    tangent_sq = jnp.sum(tangents * tangents, axis=2)
    local_curv = jnp.sum(slope * tangent_sq, axis=(1, 2)) / (PROBES * D)

    everyones = lax.all_gather(local_curv, ("xh", "z", "c"), axis=0)
    curv = jnp.sum(everyones.reshape(2, 8, 2, block), axis=1)
    curv = curv.reshape(2, 2, 2, block // 2).transpose(2, 0, 1, 3).reshape(4 * block)

    placed = primal.astype(jnp.bfloat16).transpose(1, 0, 2)
    placed = lax.all_to_all(placed, ("xh", "c"), 0, 0, tiled=True)
    placed = placed.reshape(2, 2, 2, block // 2, rows).transpose(2, 0, 1, 3, 4)
    return (placed.reshape(4 * block, rows), curv)


def solution(mesh):
    fine = Mesh(mesh.devices.reshape(tuple(AXES.values())), tuple(AXES))
    fsdp, tp = ("xh", "z", "c"), ("xl", "y")
    return jax.shard_map(
        on_device,
        mesh=fine,
        in_specs=(
            P(fsdp, tp),
            P(),
            P(fsdp, tp),
            P(fsdp, tp),
            P(fsdp, tp),
            P(None, fsdp, tp),
        ),
        out_specs=(P(tp, fsdp), P(tp)),
        check_vma=False,
    )
```

```python
import jax
import jax.numpy as jnp
from jax import lax
from jax.sharding import Mesh
from jax.sharding import PartitionSpec as P

PROBES = 2
AXES = {"xh": 2, "z": 8, "c": 2, "xl": 2, "y": 4}

epsilon = 1e-06


def moved(array, axis, shift):
    n = AXES[axis]
    return lax.ppermute(array, axis, [(i, (i + shift) % n) for i in range(n)])


def flipped(array, *axes):
    n = 2 ** len(axes)
    return lax.ppermute(array, axes, [(i, n - 1 - i) for i in range(n)])


def pick(stack, index):
    return lax.dynamic_index_in_dim(stack, index, 0, keepdims=False)


def by_index(own, other, index):
    first = index == 0
    return jnp.stack([jnp.where(first, own, other), jnp.where(first, other, own)])


def step_of_ring(down, up, axis):
    return moved(down, axis, 1), moved(up, axis, -1)


def ring(own, axis):
    got, down, up = [], own, own
    for _ in range(3):
        down, up = step_of_ring(down, up, axis)
        got.append((down, up))
    half = own.shape[0] // 2
    last = (moved(down[:half], axis, 1), moved(up[half:], axis, -1))
    return got, jnp.concatenate(last, axis=0)


def on_device(tokens, norm_gain, gate_weight, up_weight, down_weight, probes):
    xh, z, c, xl, y = (lax.axis_index(a) for a in AXES)
    rows, units = gate_weight.shape
    block, width = tokens.shape
    part = units // 4
    count = 1 + PROBES

    halves = [w.reshape(rows, 4, part).transpose(1, 0, 2) for w in (gate_weight, up_weight)]
    quarters = jnp.concatenate(halves, axis=2)
    quarter = lambda a, b: pick(quarters, 2 * a + b)
    for_core = jnp.stack([quarter(xh, 1 - c), quarter(1 - xh, 1 - c)])
    from_core = flipped(for_core, "c")
    near = by_index(quarter(xh, c), from_core[0], c).reshape(2 * rows, 2 * part)
    far = by_index(quarter(1 - xh, c), from_core[1], c).reshape(2 * rows, 2 * part)
    far = flipped(far, "xh")
    near_ring, near_last = ring(near, "z")
    far_ring, far_last = ring(far, "z")

    mine = tokens.T
    mine = jnp.concatenate([mine, flipped(mine, "xh")], axis=1)
    mine = by_index(mine, flipped(mine, "xl"), xl)
    down, up = step_of_ring(mine, mine, "y")
    across = jnp.stack([moved(down[0], "y", 1), moved(up[1], "y", -1)])
    around = jnp.stack([mine, up, across, down])
    features = jnp.stack([pick(around, (j - y) % 4) for j in range(4)], axis=1)
    features = features.reshape(8 * width, 2 * block)
    widened = features.astype(jnp.float32)
    inverse_rms = lax.rsqrt(jnp.mean(widened * widened, axis=0, keepdims=True) + epsilon)
    normed = (widened * inverse_rms * norm_gain.astype(jnp.float32)[:, None]).astype(jnp.bfloat16)
    normed = jnp.concatenate([normed, flipped(normed, "c")], axis=1)
    normed = normed.reshape(2, 8, 2 * rows, 4 * block)

    def summed_over(sources):
        left = jnp.concatenate([normed[a, b] for a, b, _ in sources], axis=0)
        right = jnp.concatenate([w for _, _, w in sources], axis=0)
        return lax.dot_general(
            left, right, (((0,), (0,)), ((), ())), preferred_element_type=jnp.float32
        )

    sums = summed_over([(xh, z, near), (1 - xh, z, far)])
    for i in range(3):
        lo, hi = (z - i - 1) % 8, (z + i + 1) % 8
        sums += summed_over(
            [
                (xh, lo, near_ring[i][0]),
                (xh, hi, near_ring[i][1]),
                (1 - xh, lo, far_ring[i][0]),
                (1 - xh, hi, far_ring[i][1]),
            ]
        )
    sums += summed_over([(xh, (z + 4) % 8, near_last), (1 - xh, (z + 4) % 8, far_last)])
    gate_sum, up_sum = sums[:, :part], sums[:, part:]
    hidden = (jax.nn.silu(gate_sum) * up_sum).astype(jnp.bfloat16)

    flat = jnp.concatenate([down_weight[None], probes], axis=0).reshape(count * rows, units)
    half = count * rows // 2
    next_xl, next_x = flipped(flat, "xl"), flipped(flat, "xh", "xl")
    next_xh = jnp.concatenate(
        [flipped(next_x[:half], "xl"), flipped(next_xl[half:], "xh", "xl")], axis=0
    )
    own_units = jnp.concatenate([flat, next_xh], axis=0)
    other_units = jnp.concatenate([next_xl, next_x], axis=0)
    own_units = jnp.concatenate([own_units, flipped(own_units, "c")], axis=0)
    other_units = jnp.concatenate([other_units, flipped(other_units, "c")], axis=0)
    matrices = jnp.concatenate([own_units, other_units], axis=1)

    small = block // 2
    chunks = hidden.reshape(4, 2, small, part)
    chunks = jnp.stack(
        [pick(chunks, 2 * (c ^ c_t) + (xh ^ xh_t)) for c_t in (0, 1) for xh_t in (0, 1)]
    )
    chunks = chunks.reshape(8, small, part)
    arrived = lax.all_to_all(chunks, ("xh", "xl", "c"), 0, 0, tiled=True)
    arrived = arrived.reshape(2, 2, 2, small, part)
    arrived = jnp.moveaxis(arrived, 1, 0)
    arrived = jnp.stack([pick(arrived, xl), pick(arrived, 1 - xl)])
    shard = arrived.transpose(3, 0, 1, 2, 4).reshape(small, 2 * units)

    def product(tok):
        return lax.dot_general(
            tok, matrices, (((1,), (1,)), ((), ())), preferred_element_type=jnp.float32
        ).astype(jnp.bfloat16)

    hidden_ring, hidden_last = ring(shard, "z")
    outs = [product(jnp.concatenate(pair, axis=0)) for pair in hidden_ring]
    ends = product(jnp.concatenate([shard, hidden_last], axis=0))
    lo = [o[:small] for o in outs]
    hi = [o[small:] for o in outs]
    terms = jnp.stack([ends[:small], *hi, ends[small:], lo[2], lo[1], lo[0]])

    def terms_for(shift):
        first = 2 * ((y + shift) % 4)
        return jnp.concatenate([pick(terms, (first + i - z) % 8) for i in (0, 1)], axis=0)

    wide = lambda a: a.astype(jnp.float32)
    two_on = terms_for(2)
    for_next, for_last = moved(two_on[:small], "y", 1), moved(two_on[small:], "y", -1)
    next_one, last_one = terms_for(1), terms_for(3)
    top = (wide(next_one[:small]) + wide(for_next)).astype(jnp.bfloat16)
    bottom = (wide(last_one[small:]) + wide(for_last)).astype(jnp.bfloat16)
    from_last = moved(jnp.concatenate([top, next_one[small:]], axis=0), "y", 1)
    from_next = moved(jnp.concatenate([last_one[:small], bottom], axis=0), "y", -1)
    summed = wide(terms_for(0)) + wide(from_last) + wide(from_next)

    summed = summed.reshape(block, 4, count, rows)
    primal = summed[:, :, 0]
    tangents = summed[:, :, 1:]
    squashed = jax.nn.sigmoid(primal)
    slope = squashed * (1.0 - squashed)
    tangent_sq = jnp.sum(tangents * tangents, axis=2)
    local_curv = jnp.sum(slope * tangent_sq, axis=(1, 2)) / (PROBES * 32 * rows)

    spread = jnp.broadcast_to(local_curv[None, None], (32, 1, block))
    everyones = lax.all_to_all(spread, ("xh", "z", "c"), 0, 0, tiled=True)
    curv = jnp.sum(everyones.reshape(2, 8, 2, block), axis=1)
    curv = curv.reshape(2, 2, 2, small).transpose(2, 0, 1, 3).reshape(4 * block)

    placed = primal.astype(jnp.bfloat16).transpose(1, 0, 2)
    placed = [
        placed[0],
        flipped(placed[1], "xh"),
        flipped(placed[2], "c"),
        flipped(placed[3], "xh", "c"),
    ]
    placed = jnp.stack(placed)
    placed = jnp.stack([pick(placed, 2 * (c ^ h) + (xh ^ t)) for t in (0, 1) for h in (0, 1)])
    placed = placed.reshape(4, 2, small, rows).transpose(1, 0, 2, 3)
    return (placed.reshape(4 * block, rows), curv)


def solution(mesh):
    fine = Mesh(mesh.devices.reshape(tuple(AXES.values())), tuple(AXES))
    fsdp, tp = ("xh", "z", "c"), ("xl", "y")
    return jax.shard_map(
        on_device,
        mesh=fine,
        in_specs=(
            P(fsdp, tp),
            P(),
            P(fsdp, tp),
            P(fsdp, tp),
            P(fsdp, tp),
            P(None, fsdp, tp),
        ),
        out_specs=(P(tp, fsdp), P(tp)),
        check_vma=False,
    )
```

```python
import jax
import jax.numpy as jnp
from jax import lax
from jax.sharding import Mesh
from jax.sharding import PartitionSpec as P

PROBES = 2
AXES = {"xh": 2, "z": 8, "c": 2, "xl": 2, "y": 4}

epsilon = 1e-06


def moved(array, axis, shift):
    n = AXES[axis]
    return lax.ppermute(array, axis, [(i, (i + shift) % n) for i in range(n)])


def flipped(array, *axes):
    n = 2 ** len(axes)
    return lax.ppermute(array, axes, [(i, n - 1 - i) for i in range(n)])


def pick(stack, index):
    return lax.dynamic_index_in_dim(stack, index, 0, keepdims=False)


def by_index(own, other, index):
    first = index == 0
    return jnp.stack([jnp.where(first, own, other), jnp.where(first, other, own)])


def after(array, *others):
    return lax.optimization_barrier((array, *others))[0]


def step_of_ring(down, up, axis):
    return moved(down, axis, 1), moved(up, axis, -1)


def ring(own, axis):
    got, down, up = [], own, own
    for _ in range(3):
        down, up = step_of_ring(down, up, axis)
        got.append((down, up))
    half = own.shape[0] // 2
    last = (moved(down[:half], axis, 1), moved(up[half:], axis, -1))
    return got, jnp.concatenate(last, axis=0)


def on_device(tokens, norm_gain, gate_weight, up_weight, down_weight, probes):
    xh, z, c, xl, y = (lax.axis_index(a) for a in AXES)
    rows, units = gate_weight.shape
    block, width = tokens.shape
    part = units // 4
    count = 1 + PROBES

    mine = tokens.T
    partner = flipped(mine, "xh")
    halves = [w.reshape(rows, 4, part).transpose(1, 0, 2) for w in (gate_weight, up_weight)]
    quarters = jnp.concatenate(halves, axis=2)
    quarter = lambda a, b: pick(quarters, 2 * a + b)
    for_core = jnp.stack([quarter(xh, 1 - c), quarter(1 - xh, 1 - c)])
    from_core = flipped(for_core, "c")
    near = by_index(quarter(xh, c), from_core[0], c).reshape(2 * rows, 2 * part)
    far = by_index(quarter(1 - xh, c), from_core[1], c).reshape(2 * rows, 2 * part)
    far = flipped(far, "xh")
    near_ring, near_last = ring(near, "z")
    far_ring, far_last = ring(far, "z")

    mine = after(jnp.concatenate([mine, partner], axis=1), from_core)
    mine = by_index(mine, flipped(mine, "xl"), xl)
    spread = after(jnp.broadcast_to(mine[None], (4, 2, width, 2 * block)), far)
    features = jnp.moveaxis(lax.all_to_all(spread, "y", 0, 0, tiled=True), 0, 1)
    features = features.reshape(8 * width, 2 * block)
    widened = features.astype(jnp.float32)
    inverse_rms = lax.rsqrt(jnp.mean(widened * widened, axis=0, keepdims=True) + epsilon)
    normed = (widened * inverse_rms * norm_gain.astype(jnp.float32)[:, None]).astype(jnp.bfloat16)
    normed = jnp.concatenate([normed, flipped(normed, "c")], axis=1)
    normed = normed.reshape(2, 8, 2 * rows, 4 * block)
    normed = jnp.stack([pick(normed, xh), pick(normed, 1 - xh)], axis=1)
    normed = jnp.stack([pick(normed, (z + i) % 8) for i in range(8)])

    flat = jnp.concatenate([down_weight[None], probes], axis=0).reshape(count * rows, units)
    half = count * rows // 2
    flat = after(flat, far)
    next_xl, next_x = flipped(flat, "xl"), flipped(flat, "xh", "xl")
    next_xh = jnp.concatenate(
        [flipped(next_x[:half], "xl"), flipped(next_xl[half:], "xh", "xl")], axis=0
    )
    own_units = jnp.concatenate([flat, next_xh], axis=0)
    other_units = jnp.concatenate([next_xl, next_x], axis=0)
    own_units = jnp.concatenate([own_units, flipped(own_units, "c")], axis=0)
    other_units = jnp.concatenate([other_units, flipped(other_units, "c")], axis=0)

    far_last, normed, own_units, other_units = lax.optimization_barrier(
        (far_last, normed, own_units, other_units)
    )
    nears = [near, *[r[1] for r in near_ring], near_last, *[r[0] for r in near_ring[::-1]]]
    fars = [far, *[r[1] for r in far_ring], far_last, *[r[0] for r in far_ring[::-1]]]
    weights = jnp.concatenate([w for pair in zip(nears, fars) for w in pair], axis=0)
    normed = normed.reshape(32 * rows, 4 * block)
    sums = lax.dot_general(
        normed, weights, (((0,), (0,)), ((), ())), preferred_element_type=jnp.float32
    )
    gate_sum, up_sum = sums[:, :part], sums[:, part:]
    hidden = (jax.nn.silu(gate_sum) * up_sum).astype(jnp.bfloat16)

    small = block // 2
    chunks = hidden.reshape(4, 2, small, part)
    chunks = jnp.stack(
        [pick(chunks, 2 * (c ^ c_t) + (xh ^ xh_t)) for c_t in (0, 1) for xh_t in (0, 1)]
    )
    chunks = chunks.reshape(8, small, part)
    arrived = lax.all_to_all(chunks, ("xh", "xl", "c"), 0, 0, tiled=True)
    arrived = arrived.reshape(2, 2, 2, small, part)
    arrived = jnp.moveaxis(arrived, 1, 0)
    arrived = jnp.stack([pick(arrived, xl), pick(arrived, 1 - xl)])
    shard = arrived.transpose(3, 0, 1, 2, 4).reshape(small, 2 * units)

    def product(tok):
        first, second = [
            lax.dot_general(t, m, (((1,), (1,)), ((), ())), preferred_element_type=jnp.float32)
            for t, m in ((tok[:, :units], own_units), (tok[:, units:], other_units))
        ]
        return (first + second).astype(jnp.bfloat16)

    hidden_ring, hidden_last = ring(shard, "z")
    outs = [product(jnp.concatenate(pair, axis=0)) for pair in hidden_ring]
    ends = product(jnp.concatenate([shard, hidden_last], axis=0))
    lo = [o[:small] for o in outs]
    hi = [o[small:] for o in outs]
    terms = jnp.stack([ends[:small], *hi, ends[small:], lo[2], lo[1], lo[0]])

    def terms_for(shift):
        first = 2 * ((y + shift) % 4)
        return jnp.concatenate([pick(terms, (first + i - z) % 8) for i in (0, 1)], axis=0)

    wide = lambda a: a.astype(jnp.float32)
    two_on = terms_for(2)
    for_next, for_last = moved(two_on[:small], "y", 1), moved(two_on[small:], "y", -1)
    next_one, last_one = terms_for(1), terms_for(3)
    top = (wide(next_one[:small]) + wide(for_next)).astype(jnp.bfloat16)
    bottom = (wide(last_one[small:]) + wide(for_last)).astype(jnp.bfloat16)
    from_last = moved(jnp.concatenate([top, next_one[small:]], axis=0), "y", 1)
    from_next = moved(jnp.concatenate([last_one[:small], bottom], axis=0), "y", -1)
    summed = wide(terms_for(0)) + wide(from_last) + wide(from_next)

    summed = summed.reshape(block, 4, count, rows)
    primal = summed[:, :, 0]
    tangents = summed[:, :, 1:]
    squashed = jax.nn.sigmoid(primal)
    slope = squashed * (1.0 - squashed)
    tangent_sq = jnp.sum(tangents * tangents, axis=2)
    local_curv = jnp.sum(slope * tangent_sq, axis=(1, 2)) / (PROBES * 32 * rows)

    spread = jnp.broadcast_to(local_curv[None, None], (32, 1, block))
    everyones = lax.all_to_all(spread, ("xh", "z", "c"), 0, 0, tiled=True)
    curv = jnp.sum(everyones.reshape(2, 8, 2, block), axis=1)
    curv = curv.reshape(2, 2, 2, small).transpose(2, 0, 1, 3).reshape(4 * block)

    placed = primal.astype(jnp.bfloat16).transpose(1, 0, 2)
    placed = [
        placed[0],
        flipped(placed[1], "xh"),
        flipped(placed[2], "c"),
        flipped(placed[3], "xh", "c"),
    ]
    placed = jnp.stack(placed)
    placed = jnp.stack([pick(placed, 2 * (c ^ h) + (xh ^ t)) for t in (0, 1) for h in (0, 1)])
    placed = placed.reshape(4, 2, small, rows).transpose(1, 0, 2, 3)
    return (placed.reshape(4 * block, rows), curv)


def solution(mesh):
    fine = Mesh(mesh.devices.reshape(tuple(AXES.values())), tuple(AXES))
    fsdp, tp = ("xh", "z", "c"), ("xl", "y")
    return jax.shard_map(
        on_device,
        mesh=fine,
        in_specs=(
            P(fsdp, tp),
            P(),
            P(fsdp, tp),
            P(fsdp, tp),
            P(fsdp, tp),
            P(None, fsdp, tp),
        ),
        out_specs=(P(tp, fsdp), P(tp)),
        check_vma=False,
    )
```

```python
import jax
import jax.numpy as jnp
from jax import lax
from jax.sharding import Mesh
from jax.sharding import PartitionSpec as P

PROBES = 2
AXES = {"xh": 2, "z": 8, "c": 2, "xl": 2, "y": 4}

epsilon = 1e-06


def moved(array, axis, shift):
    n = AXES[axis]
    return lax.ppermute(array, axis, [(i, (i + shift) % n) for i in range(n)])


def flipped(array, *axes):
    n = 2 ** len(axes)
    return lax.ppermute(array, axes, [(i, n - 1 - i) for i in range(n)])


def pick(stack, index):
    return lax.dynamic_index_in_dim(stack, index, 0, keepdims=False)


def by_index(own, other, index):
    first = index == 0
    return jnp.stack([jnp.where(first, own, other), jnp.where(first, other, own)])


def after(array, *others):
    return lax.optimization_barrier((array, *others))[0]


def ring(own, axis, gates=None):
    got, down, up = [], own, own
    for i in range(3):
        if i:
            down, up = lax.optimization_barrier((down, up, *(gates or {}).get(i, ())))[:2]
        down = moved(down, axis, 1)
        up = moved(up, axis, -1)
        got.append((down, up))
    down, up = lax.optimization_barrier((down, up))
    half = own.shape[0] // 2
    top = moved(down[:half], axis, 1)
    bottom = moved(up[half:], axis, -1)
    return got, jnp.concatenate((top, bottom), axis=0)


def on_device(tokens, norm_gain, gate_weight, up_weight, down_weight, probes):
    xh, z, c, xl, _ = (lax.axis_index(a) for a in AXES)
    rows, units = gate_weight.shape
    block, width = tokens.shape
    part = units // 4
    count = 1 + PROBES

    halves = [w.reshape(rows, 4, part).transpose(1, 0, 2) for w in (gate_weight, up_weight)]
    quarters = jnp.concatenate(halves, axis=2)
    quarter = lambda a, b: pick(quarters, 2 * a + b)
    for_core = jnp.stack([quarter(xh, 1 - c), quarter(1 - xh, 1 - c)])
    from_core = flipped(for_core, "c")
    near = by_index(quarter(xh, c), from_core[0], c).reshape(2 * rows, 2 * part)
    far = by_index(quarter(1 - xh, c), from_core[1], c).reshape(2 * rows, 2 * part)
    far = flipped(far, "xh")
    near = jnp.concatenate([near, far], axis=0)

    flat = jnp.concatenate([down_weight[None], probes], axis=0).reshape(count * rows, units)
    flat = after(flat, far)
    next_xl = flipped(flat, "xl")
    next_x = flipped(flat, "xh", "xl")
    weight_ring, weight_last = ring(near, "z", {2: (next_xl, next_x)})
    next_xh = flipped(after(flat, weight_ring[0][0]), "xh")
    spread = after(jnp.broadcast_to(tokens.T[None], (4, width, block)), for_core)
    row = lax.all_to_all(spread, ("xh", "xl"), 0, 0, tiled=True)
    spread = jnp.broadcast_to(row[None], (4, 4, width, block))
    plane = lax.all_to_all(spread, "y", 0, 0, tiled=True)
    plane = after(plane, *weight_ring[1]).reshape(4, 2, 2, width, block)
    features = plane.transpose(2, 0, 3, 1, 4).reshape(8 * width, 2 * block)
    widened = features.astype(jnp.float32)
    inverse_rms = lax.rsqrt(jnp.mean(widened * widened, axis=0, keepdims=True) + epsilon)
    normed = (widened * inverse_rms * norm_gain.astype(jnp.float32)[:, None]).astype(jnp.bfloat16)
    partner = flipped(normed, "c")
    normed = jnp.concatenate([normed, partner], axis=1)
    normed = normed.reshape(2, 8, 2 * rows, 4 * block)
    normed = jnp.stack([pick(normed, xh), pick(normed, 1 - xh)], axis=1)
    normed = normed.reshape(8, 4 * rows, 4 * block)

    weight_last, next_xh = lax.optimization_barrier((weight_last, next_xh))
    own_rows = jnp.concatenate([flat, next_xh, next_xl, next_x], axis=0)
    own_rows = own_rows.reshape(2, 2 * count * rows, units)
    matrices = (own_rows, flipped(own_rows, "c"))

    def summed_over(blocks):
        left = jnp.concatenate([pick(normed, (z + i) % 8) for i, _ in blocks], axis=0)
        right = jnp.concatenate([w for _, w in blocks], axis=0)
        return lax.dot_general(
            left, right, (((0,), (0,)), ((), ())), preferred_element_type=jnp.float32
        )

    sums = summed_over([(0, near)])
    for i, (down, up) in enumerate(weight_ring):
        sums += summed_over([(7 - i, down), (i + 1, up)])
    sums += summed_over([(4, weight_last)])
    gate_sum, up_sum = sums[:, :part], sums[:, part:]
    hidden = (jax.nn.silu(gate_sum) * up_sum).astype(jnp.bfloat16)

    small = block // 2
    chunks = hidden.reshape(4, 2, small, part)
    chunks = jnp.stack(
        [pick(chunks, 2 * (c ^ c_t) + xh_t) for c_t in (0, 1) for xh_t in (0, 1)]
    )
    chunks = chunks.reshape(8, small, part)
    arrived = lax.all_to_all(chunks, ("xh", "xl", "c"), 0, 0, tiled=True)
    arrived = arrived.reshape(2, 2, 2, small, part)
    arrived = jnp.moveaxis(arrived, 1, 0)
    arrived = jnp.stack([pick(arrived, xl), pick(arrived, 1 - xl)])
    shard = arrived.transpose(3, 0, 1, 2, 4).reshape(small, 2 * units)

    def with_products(terms, blocks, places):
        tok = jnp.concatenate(blocks, axis=0)
        parts = []
        for m in matrices:
            first, second = [
                lax.dot_general(t, u, (((1,), (1,)), ((), ())), preferred_element_type=jnp.float32)
                for t, u in ((tok[:, :units], m[0]), (tok[:, units:], m[1]))
            ]
            parts.append((first + second).astype(jnp.bfloat16))
        out = jnp.concatenate(parts, axis=1)
        for place, o in zip(places, (out[:small], out[small:])):
            terms = lax.dynamic_update_index_in_dim(terms, o, place % 8, 0)
        return terms

    def step(i, carry):
        down, up, terms = carry
        later = moved(down, "z", 1), moved(up, "z", -1)
        return *later, with_products(terms, (down, up), (z - i + 8, z + i))

    terms = jnp.zeros((8, small, 4 * count * rows), jnp.bfloat16)
    down, up, terms = lax.fori_loop(0, 3, step, (shard, shard, terms))
    top = moved(down[: small // 2], "z", 1)
    bottom = moved(up[small // 2 :], "z", -1)
    terms = with_products(terms, (down, up), (z + 5, z + 3))
    across = jnp.concatenate([top, bottom], axis=0)
    terms = with_products(terms, (across, across), (z + 4, z + 4))

    terms = terms.reshape(4, block, -1)
    terms = lax.all_to_all(terms, "y", 0, 0, tiled=True)
    summed = jnp.sum(terms.astype(jnp.float32), axis=0)

    summed = summed.reshape(block, 4, count, rows)
    primal = summed[:, :, 0]
    tangents = summed[:, :, 1:]
    squashed = jax.nn.sigmoid(primal)
    slope = squashed * (1.0 - squashed)
    tangent_sq = jnp.sum(tangents * tangents, axis=2)
    local_curv = jnp.sum(slope * tangent_sq, axis=(1, 2)) / (PROBES * 32 * rows)

    spread = jnp.broadcast_to(local_curv[None, None], (32, 1, block))
    everyones = lax.all_to_all(spread, ("xh", "z", "c"), 0, 0, tiled=True)
    curv = jnp.sum(everyones.reshape(2, 8, 2, block), axis=1)
    curv = curv.reshape(2, 2, 2, small).transpose(2, 0, 1, 3).reshape(4 * block)

    placed = primal.astype(jnp.bfloat16).transpose(1, 0, 2)
    placed = jnp.stack([pick(placed, 2 * (c ^ j) + (xh ^ i)) for i in (0, 1) for j in (0, 1)])
    placed = lax.all_to_all(placed, ("xh", "c"), 0, 0, tiled=True)
    placed = placed.reshape(4, 2, small, rows).transpose(1, 0, 2, 3)
    return (placed.reshape(4 * block, rows), curv)


def solution(mesh):
    def step(*arrays):
        return on_device(*arrays)

    fine = Mesh(mesh.devices.reshape(tuple(AXES.values())), tuple(AXES))
    fsdp, tp = ("xh", "z", "c"), ("xl", "y")
    step = jax.shard_map(
        step,
        mesh=fine,
        in_specs=(
            P(fsdp, tp),
            P(),
            P(fsdp, tp),
            P(fsdp, tp),
            P(fsdp, tp),
            P(None, fsdp, tp),
        ),
        out_specs=(P(tp, fsdp), P(tp)),
        check_vma=False,
    )
    return step
```

```python
import jax
import jax.numpy as jnp
from jax import lax
from jax.sharding import Mesh
from jax.sharding import PartitionSpec as P

PROBES = 2
AXES = {"xh": 2, "z": 8, "c": 2, "xl": 2, "y": 4}

epsilon = 1e-06


def moved(array, axis, shift):
    n = AXES[axis]
    return lax.ppermute(array, axis, [(i, (i + shift) % n) for i in range(n)])


def flipped(array, *axes):
    n = 2 ** len(axes)
    return lax.ppermute(array, axes, [(i, n - 1 - i) for i in range(n)])


def pick(stack, index):
    return lax.dynamic_index_in_dim(stack, index, 0, keepdims=False)


def by_index(own, other, index):
    first = index == 0
    return jnp.stack([jnp.where(first, own, other), jnp.where(first, other, own)])


def after(array, *others):
    return lax.optimization_barrier((array, *others))[0]


def ring(own, axis, gates=None):
    got, down, up = [], own, own
    for i in range(3):
        if i:
            down, up = lax.optimization_barrier((down, up, *(gates or {}).get(i, ())))[:2]
        down = moved(down, axis, 1)
        up = moved(up, axis, -1)
        got.append((down, up))
    down, up = lax.optimization_barrier((down, up))
    half = own.shape[0] // 2
    top = moved(down[:half], axis, 1)
    bottom = moved(up[half:], axis, -1)
    return got, jnp.concatenate((top, bottom), axis=0)


def on_device(tokens, norm_gain, gate_weight, up_weight, down_weight, probes):
    xh, z, c, xl, y = (lax.axis_index(a) for a in AXES)
    rows, units = gate_weight.shape
    block, width = tokens.shape
    part = units // 4
    count = 1 + PROBES

    mine = tokens.T
    partner = flipped(mine, "xh")
    halves = [w.reshape(rows, 4, part).transpose(1, 0, 2) for w in (gate_weight, up_weight)]
    quarters = jnp.concatenate(halves, axis=2)
    quarter = lambda a, b: pick(quarters, 2 * a + b)
    for_core = jnp.stack([quarter(xh, 1 - c), quarter(1 - xh, 1 - c)])
    from_core = flipped(for_core, "c")
    near = by_index(quarter(xh, c), from_core[0], c).reshape(2 * rows, 2 * part)
    far = by_index(quarter(1 - xh, c), from_core[1], c).reshape(2 * rows, 2 * part)
    far = flipped(far, "xh")
    near = jnp.concatenate([near, far], axis=0)

    flat = jnp.concatenate([down_weight[None], probes], axis=0).reshape(count * rows, units)
    flat = after(flat, far)
    next_xl = flipped(flat, "xl")
    next_x = flipped(flat, "xh", "xl")
    weight_ring, weight_last = ring(near, "z", {2: (next_xl, next_x)})
    next_xh = flipped(after(flat, weight_ring[0][0]), "xh")
    mine = after(jnp.concatenate([mine, partner], axis=1), from_core)
    mine = by_index(mine, flipped(mine, "xl"), xl)
    spread = jnp.broadcast_to(mine[None], (4, 2, width, 2 * block))
    features = jnp.moveaxis(lax.all_to_all(spread, "y", 0, 0, tiled=True), 0, 1)
    features = features.reshape(8 * width, 2 * block)
    features = after(features, *weight_ring[1])
    widened = features.astype(jnp.float32)
    inverse_rms = lax.rsqrt(jnp.mean(widened * widened, axis=0, keepdims=True) + epsilon)
    normed = (widened * inverse_rms * norm_gain.astype(jnp.float32)[:, None]).astype(jnp.bfloat16)
    partner = flipped(normed, "c")
    normed = jnp.concatenate([normed, partner], axis=1)
    normed = normed.reshape(2, 8, 2 * rows, 4 * block)
    normed = jnp.stack([pick(normed, xh), pick(normed, 1 - xh)], axis=1)
    normed = normed.reshape(8, 4 * rows, 4 * block)

    weight_last, next_xh = lax.optimization_barrier((weight_last, next_xh))
    own_units = jnp.concatenate([flat, next_xh], axis=0)
    other_units = jnp.concatenate([next_xl, next_x], axis=0)
    own_units = jnp.concatenate([own_units, flipped(own_units, "c")], axis=0)
    other_units = jnp.concatenate([other_units, flipped(other_units, "c")], axis=0)

    def summed_over(blocks):
        left = jnp.concatenate([pick(normed, (z + i) % 8) for i, _ in blocks], axis=0)
        right = jnp.concatenate([w for _, w in blocks], axis=0)
        return lax.dot_general(
            left, right, (((0,), (0,)), ((), ())), preferred_element_type=jnp.float32
        )

    sums = summed_over([(0, near)])
    for i, (down, up) in enumerate(weight_ring):
        sums += summed_over([(7 - i, down), (i + 1, up)])
    sums += summed_over([(4, weight_last)])
    gate_sum, up_sum = sums[:, :part], sums[:, part:]
    hidden = (jax.nn.silu(gate_sum) * up_sum).astype(jnp.bfloat16)

    small = block // 2
    chunks = hidden.reshape(4, 2, small, part)
    chunks = jnp.stack(
        [pick(chunks, 2 * (c ^ c_t) + (xh ^ xh_t)) for c_t in (0, 1) for xh_t in (0, 1)]
    )
    chunks = chunks.reshape(8, small, part)
    arrived = lax.all_to_all(chunks, ("xh", "xl", "c"), 0, 0, tiled=True)
    arrived = arrived.reshape(2, 2, 2, small, part)
    arrived = jnp.moveaxis(arrived, 1, 0)
    arrived = jnp.stack([pick(arrived, xl), pick(arrived, 1 - xl)])
    shard = arrived.transpose(3, 0, 1, 2, 4).reshape(small, 2 * units)

    def product(blocks):
        tok = jnp.concatenate(blocks, axis=0)
        first, second = [
            lax.dot_general(t, m, (((1,), (1,)), ((), ())), preferred_element_type=jnp.float32)
            for t, m in ((tok[:, :units], own_units), (tok[:, units:], other_units))
        ]
        return (first + second).astype(jnp.bfloat16)

    hidden_ring, hidden_last = ring(shard, "z")
    outs = [product(pair) for pair in hidden_ring]
    ends = product((shard, hidden_last))
    lo = [o[:small] for o in outs]
    hi = [o[small:] for o in outs]
    terms = jnp.stack([ends[:small], *hi, ends[small:], lo[2], lo[1], lo[0]])

    def terms_for(shift):
        first = 2 * ((y + shift) % 4)
        return jnp.concatenate([pick(terms, (first + i - z) % 8) for i in (0, 1)], axis=0)

    wide = lambda a: a.astype(jnp.float32)
    half = 2 * count * rows
    two_on = terms_for(2)
    for_next, for_last = moved(two_on[:, :half], "y", 1), moved(two_on[:, half:], "y", -1)
    next_one, last_one = terms_for(1), terms_for(3)
    left = (wide(next_one[:, :half]) + wide(for_next)).astype(jnp.bfloat16)
    right = (wide(last_one[:, half:]) + wide(for_last)).astype(jnp.bfloat16)
    from_last = moved(jnp.concatenate([left, next_one[:, half:]], axis=1), "y", 1)
    from_next = moved(jnp.concatenate([last_one[:, :half], right], axis=1), "y", -1)
    summed = wide(terms_for(0)) + wide(from_last) + wide(from_next)

    summed = summed.reshape(block, 4, count, rows)
    primal = summed[:, :, 0]
    tangents = summed[:, :, 1:]
    squashed = jax.nn.sigmoid(primal)
    slope = squashed * (1.0 - squashed)
    tangent_sq = jnp.sum(tangents * tangents, axis=2)
    local_curv = jnp.sum(slope * tangent_sq, axis=(1, 2)) / (PROBES * 32 * rows)

    spread = jnp.broadcast_to(local_curv[None, None], (32, 1, block))
    everyones = lax.all_to_all(spread, ("xh", "z", "c"), 0, 0, tiled=True)
    curv = jnp.sum(everyones.reshape(2, 8, 2, block), axis=1)
    curv = curv.reshape(2, 2, 2, small).transpose(2, 0, 1, 3).reshape(4 * block)

    placed = primal.astype(jnp.bfloat16).transpose(1, 0, 2)
    placed = [
        placed[0],
        flipped(placed[1], "xh"),
        flipped(placed[2], "c"),
        flipped(placed[3], "xh", "c"),
    ]
    placed = jnp.stack(placed)
    placed = jnp.stack([pick(placed, 2 * (c ^ h) + (xh ^ t)) for t in (0, 1) for h in (0, 1)])
    placed = placed.reshape(4, 2, small, rows).transpose(1, 0, 2, 3)
    return (placed.reshape(4 * block, rows), curv)


def solution(mesh):
    def step(*arrays):
        return on_device(*arrays)

    fine = Mesh(mesh.devices.reshape(tuple(AXES.values())), tuple(AXES))
    fsdp, tp = ("xh", "z", "c"), ("xl", "y")
    step = jax.shard_map(
        step,
        mesh=fine,
        in_specs=(
            P(fsdp, tp),
            P(),
            P(fsdp, tp),
            P(fsdp, tp),
            P(fsdp, tp),
            P(None, fsdp, tp),
        ),
        out_specs=(P(tp, fsdp), P(tp)),
        check_vma=False,
    )
    return step
```

```python
import jax
import jax.numpy as jnp
from jax import lax
from jax.sharding import Mesh
from jax.sharding import PartitionSpec as P

PROBES = 2
AXES = {"xh": 2, "z": 8, "c": 2, "xl": 2, "y": 4}

epsilon = 1e-06


def moved(array, axis, shift):
    n = AXES[axis]
    return lax.ppermute(array, axis, [(i, (i + shift) % n) for i in range(n)])


def flipped(array, *axes):
    n = 2 ** len(axes)
    return lax.ppermute(array, axes, [(i, n - 1 - i) for i in range(n)])


def pick(stack, index):
    return lax.dynamic_index_in_dim(stack, index, 0, keepdims=False)


def by_index(own, other, index):
    first = index == 0
    return jnp.stack([jnp.where(first, own, other), jnp.where(first, other, own)])


def after(array, *others):
    return lax.optimization_barrier((array, *others))[0]


def ring(own, axis, gates=None):
    got, down, up = [], own, own
    for i in range(3):
        if i:
            down, up = lax.optimization_barrier((down, up, *(gates or {}).get(i, ())))[:2]
        down = moved(down, axis, 1)
        up = moved(up, axis, -1)
        got.append((down, up))
    down, up = lax.optimization_barrier((down, up))
    half = own.shape[0] // 2
    top = moved(down[:half], axis, 1)
    bottom = moved(up[half:], axis, -1)
    return got, jnp.concatenate((top, bottom), axis=0)


def on_device(tokens, norm_gain, gate_weight, up_weight, down_weight, probes):
    xh, z, c, xl, y = (lax.axis_index(a) for a in AXES)
    rows, units = gate_weight.shape
    block, width = tokens.shape
    part = units // 4
    count = 1 + PROBES

    mine = tokens.T
    partner = flipped(mine, "xh")
    halves = [w.reshape(rows, 4, part).transpose(1, 0, 2) for w in (gate_weight, up_weight)]
    quarters = jnp.concatenate(halves, axis=2)
    quarter = lambda a, b: pick(quarters, 2 * a + b)
    for_core = jnp.stack([quarter(xh, 1 - c), quarter(1 - xh, 1 - c)])
    from_core = flipped(for_core, "c")
    near = by_index(quarter(xh, c), from_core[0], c).reshape(2 * rows, 2 * part)
    far = by_index(quarter(1 - xh, c), from_core[1], c).reshape(2 * rows, 2 * part)
    far = flipped(far, "xh")
    near = jnp.concatenate([near, far], axis=0)

    flat = jnp.concatenate([down_weight[None], probes], axis=0).reshape(count * rows, units)
    flat = after(flat, far)
    next_xl = flipped(flat, "xl")
    next_x = flipped(flat, "xh", "xl")
    weight_ring, weight_last = ring(near, "z")
    next_xh = flipped(after(flat, weight_ring[0][0]), "xh")
    mine = after(jnp.concatenate([mine, partner], axis=1), far)
    partner = flipped(mine, "xl")
    mine = by_index(mine, partner, xl)
    spread = jnp.broadcast_to(mine[None], (4, 2, width, 2 * block))
    features = jnp.moveaxis(lax.all_to_all(spread, "y", 0, 0, tiled=True), 0, 1)
    features = features.reshape(8 * width, 2 * block)
    features = after(features, *weight_ring[1])
    widened = features.astype(jnp.float32)
    inverse_rms = lax.rsqrt(jnp.mean(widened * widened, axis=0, keepdims=True) + epsilon)
    normed = (widened * inverse_rms * norm_gain.astype(jnp.float32)[:, None]).astype(jnp.bfloat16)
    partner = flipped(normed, "c")
    normed = jnp.concatenate([normed, partner], axis=1)
    normed = normed.reshape(2, 8, 2 * rows, 4 * block)
    normed = jnp.stack([pick(normed, xh), pick(normed, 1 - xh)], axis=1)
    normed = normed.reshape(8, 4 * rows, 4 * block)

    flat, next_xl, next_x = lax.optimization_barrier((flat, next_xl, next_x, *weight_ring[2]))[:3]
    weight_last, next_xh = lax.optimization_barrier((weight_last, next_xh))
    own_units = jnp.concatenate([flat, next_xh], axis=0)
    other_units = jnp.concatenate([next_xl, next_x], axis=0)
    own_units = jnp.concatenate([own_units, flipped(own_units, "c")], axis=0)
    other_units = jnp.concatenate([other_units, flipped(other_units, "c")], axis=0)

    def summed_over(blocks):
        left = jnp.concatenate([pick(normed, (z + i) % 8) for i, _ in blocks], axis=0)
        right = jnp.concatenate([w for _, w in blocks], axis=0)
        return lax.dot_general(
            left, right, (((0,), (0,)), ((), ())), preferred_element_type=jnp.float32
        )

    sums = summed_over([(0, near)])
    for i, (down, up) in enumerate(weight_ring):
        sums += summed_over([(7 - i, down), (i + 1, up)])
    sums += summed_over([(4, weight_last)])
    gate_sum, up_sum = sums[:, :part], sums[:, part:]
    hidden = (jax.nn.silu(gate_sum) * up_sum).astype(jnp.bfloat16)

    small = block // 2
    chunks = hidden.reshape(4, 2, small, part)
    chunks = jnp.stack(
        [pick(chunks, 2 * (c ^ c_t) + (xh ^ xh_t)) for c_t in (0, 1) for xh_t in (0, 1)]
    )
    chunks = chunks.reshape(8, small, part)
    arrived = lax.all_to_all(chunks, ("xh", "xl", "c"), 0, 0, tiled=True)
    arrived = arrived.reshape(2, 2, 2, small, part)
    arrived = jnp.moveaxis(arrived, 1, 0)
    arrived = jnp.stack([pick(arrived, xl), pick(arrived, 1 - xl)])
    shard = arrived.transpose(3, 0, 1, 2, 4).reshape(small, 2 * units)

    def with_products(terms, blocks, places):
        tok = jnp.concatenate(blocks, axis=0)
        first, second = [
            lax.dot_general(t, m, (((1,), (1,)), ((), ())), preferred_element_type=jnp.float32)
            for t, m in ((tok[:, :units], own_units), (tok[:, units:], other_units))
        ]
        out = (first + second).astype(jnp.bfloat16)
        for place, o in zip(places, (out[:small], out[small:])):
            terms = lax.dynamic_update_index_in_dim(terms, o, place % 8, 0)
        return terms

    def step(i, carry):
        down, up, terms = carry
        later = moved(down, "z", 1), moved(up, "z", -1)
        return *later, with_products(terms, (down, up), (z - i + 8, z + i))

    terms = jnp.zeros((8, small, 4 * count * rows), jnp.bfloat16)
    down, up, terms = lax.fori_loop(0, 3, step, (shard, shard, terms))
    top = moved(down[: small // 2], "z", 1)
    bottom = moved(up[small // 2 :], "z", -1)
    terms = with_products(terms, (down, up), (z + 5, z + 3))
    across = jnp.concatenate([top, bottom], axis=0)
    terms = with_products(terms, (across, across), (z + 4, z + 4))

    def terms_for(shift):
        first = 2 * ((y + shift) % 4)
        return jnp.concatenate([pick(terms, first), pick(terms, first + 1)], axis=0)

    wide = lambda a: a.astype(jnp.float32)
    half = 2 * count * rows
    two_on = terms_for(2)
    for_next, for_last = moved(two_on[:, :half], "y", 1), moved(two_on[:, half:], "y", -1)
    next_one, last_one = terms_for(1), terms_for(3)
    left = (wide(next_one[:, :half]) + wide(for_next)).astype(jnp.bfloat16)
    right = (wide(last_one[:, half:]) + wide(for_last)).astype(jnp.bfloat16)
    from_last = moved(jnp.concatenate([left, next_one[:, half:]], axis=1), "y", 1)
    from_next = moved(jnp.concatenate([last_one[:, :half], right], axis=1), "y", -1)
    summed = wide(terms_for(0)) + wide(from_last) + wide(from_next)

    summed = summed.reshape(block, 4, count, rows)
    primal = summed[:, :, 0]
    tangents = summed[:, :, 1:]
    squashed = jax.nn.sigmoid(primal)
    slope = squashed * (1.0 - squashed)
    tangent_sq = jnp.sum(tangents * tangents, axis=2)
    local_curv = jnp.sum(slope * tangent_sq, axis=(1, 2)) / (PROBES * 32 * rows)

    spread = jnp.broadcast_to(local_curv[None, None], (32, 1, block))
    everyones = lax.all_to_all(spread, ("xh", "z", "c"), 0, 0, tiled=True)
    curv = jnp.sum(everyones.reshape(2, 8, 2, block), axis=1)
    curv = curv.reshape(2, 2, 2, small).transpose(2, 0, 1, 3).reshape(4 * block)

    placed = primal.astype(jnp.bfloat16).transpose(1, 0, 2)
    placed = [
        placed[0],
        flipped(placed[1], "xh"),
        flipped(placed[2], "c"),
        flipped(placed[3], "xh", "c"),
    ]
    placed = jnp.stack(placed)
    placed = jnp.stack([pick(placed, 2 * (c ^ h) + (xh ^ t)) for t in (0, 1) for h in (0, 1)])
    placed = placed.reshape(4, 2, small, rows).transpose(1, 0, 2, 3)
    return (placed.reshape(4 * block, rows), curv)


def solution(mesh):
    def step(*arrays):
        return on_device(*arrays)

    fine = Mesh(mesh.devices.reshape(tuple(AXES.values())), tuple(AXES))
    fsdp, tp = ("xh", "z", "c"), ("xl", "y")
    step = jax.shard_map(
        step,
        mesh=fine,
        in_specs=(
            P(fsdp, tp),
            P(),
            P(fsdp, tp),
            P(fsdp, tp),
            P(fsdp, tp),
            P(None, fsdp, tp),
        ),
        out_specs=(P(tp, fsdp), P(tp)),
        check_vma=False,
    )
    return step
```

```python
import jax
import jax.numpy as jnp
from jax import lax
from jax.sharding import Mesh
from jax.sharding import PartitionSpec as P

PROBES = 2
AXES = {"xh": 2, "z": 8, "c": 2, "xl": 2, "y": 4}

epsilon = 1e-06


def moved(array, axis, shift):
    n = AXES[axis]
    return lax.ppermute(array, axis, [(i, (i + shift) % n) for i in range(n)])


def flipped(array, *axes):
    n = 2 ** len(axes)
    return lax.ppermute(array, axes, [(i, n - 1 - i) for i in range(n)])


def pick(stack, index):
    return lax.dynamic_index_in_dim(stack, index, 0, keepdims=False)


def by_index(own, other, index):
    first = index == 0
    return jnp.stack([jnp.where(first, own, other), jnp.where(first, other, own)])


def after(array, *others):
    return lax.optimization_barrier((array, *others))[0]


def ring(own, axis, gates=None):
    got, down, up = [], own, own
    for i in range(3):
        if i:
            down, up = lax.optimization_barrier((down, up, *(gates or {}).get(i, ())))[:2]
        down = moved(down, axis, 1)
        up = moved(up, axis, -1)
        got.append((down, up))
    down, up = lax.optimization_barrier((down, up))
    half = own.shape[0] // 2
    top = moved(down[:half], axis, 1)
    bottom = moved(up[half:], axis, -1)
    return got, jnp.concatenate((top, bottom), axis=0)


def on_device(tokens, norm_gain, gate_weight, up_weight, down_weight, probes):
    xh, z, c, xl, y = (lax.axis_index(a) for a in AXES)
    rows, units = gate_weight.shape
    block, width = tokens.shape
    part = units // 4
    count = 1 + PROBES

    halves = [w.reshape(rows, 4, part).transpose(1, 0, 2) for w in (gate_weight, up_weight)]
    quarters = jnp.concatenate(halves, axis=2)
    quarter = lambda a, b: pick(quarters, 2 * a + b)
    for_core = jnp.stack([quarter(xh, 1 - c), quarter(1 - xh, 1 - c)])
    from_core = flipped(for_core, "c")
    near = by_index(quarter(xh, c), from_core[0], c).reshape(2 * rows, 2 * part)
    far = by_index(quarter(1 - xh, c), from_core[1], c).reshape(2 * rows, 2 * part)
    far = flipped(far, "xh")
    near = jnp.concatenate([near, far], axis=0)

    flat = jnp.concatenate([down_weight[None], probes], axis=0).reshape(count * rows, units)
    flat = after(flat, far)
    next_xl = flipped(flat, "xl")
    next_x = flipped(flat, "xh", "xl")
    weight_ring, weight_last = ring(near, "z")
    next_xh = flipped(flat, "xh")
    spread = after(jnp.broadcast_to(tokens.T[None], (16, width, block)), far)
    features = lax.all_to_all(spread, ("xh", "xl", "y"), 0, 0, tiled=True)
    features = after(features, *weight_ring[1]).reshape(2, 8 * width, block)
    widened = features.astype(jnp.float32)
    inverse_rms = lax.rsqrt(jnp.mean(widened * widened, axis=1, keepdims=True) + epsilon)
    gain = norm_gain.astype(jnp.float32)[:, None]
    normed = (widened * inverse_rms * gain).astype(jnp.bfloat16)
    partner = flipped(normed, "c")
    normed = jnp.concatenate([normed[0], normed[1], partner[0], partner[1]], axis=1)
    normed = normed.reshape(2, 8, 2 * rows, 4 * block)
    normed = jnp.stack([pick(normed, xh), pick(normed, 1 - xh)], axis=1)
    normed = normed.reshape(8, 4 * rows, 4 * block)

    own_units = jnp.concatenate([flat, next_xh], axis=0)
    other_units = jnp.concatenate([next_xl, next_x], axis=0)
    own_units = jnp.concatenate([own_units, flipped(own_units, "c")], axis=0)
    other_units = jnp.concatenate([other_units, flipped(other_units, "c")], axis=0)

    def summed_over(blocks):
        left = jnp.concatenate([pick(normed, (z + i) % 8) for i, _ in blocks], axis=0)
        right = jnp.concatenate([w for _, w in blocks], axis=0)
        return lax.dot_general(
            left, right, (((0,), (0,)), ((), ())), preferred_element_type=jnp.float32
        )

    sums = summed_over([(0, near)])
    for i, (down, up) in enumerate(weight_ring):
        sums += summed_over([(7 - i, down), (i + 1, up)])
    sums += summed_over([(4, weight_last)])
    gate_sum, up_sum = sums[:, :part], sums[:, part:]
    hidden = (jax.nn.silu(gate_sum) * up_sum).astype(jnp.bfloat16)

    small = block // 2
    chunks = hidden.reshape(4, 2, small, part)
    chunks = jnp.stack(
        [pick(chunks, 2 * (c ^ c_t) + xh_t) for c_t in (0, 1) for xh_t in (0, 1)]
    )
    chunks = chunks.reshape(8, small, part)
    arrived = lax.all_to_all(chunks, ("xh", "xl", "c"), 0, 0, tiled=True)
    arrived = arrived.reshape(2, 2, 2, small, part)
    arrived = jnp.moveaxis(arrived, 1, 0)
    arrived = jnp.stack([pick(arrived, xl), pick(arrived, 1 - xl)])
    shard = arrived.transpose(3, 0, 1, 2, 4).reshape(small, 2 * units)

    def product(blocks):
        tok = jnp.concatenate(blocks, axis=0)
        first, second = [
            lax.dot_general(t, m, (((1,), (1,)), ((), ())), preferred_element_type=jnp.float32)
            for t, m in ((tok[:, :units], own_units), (tok[:, units:], other_units))
        ]
        return (first + second).astype(jnp.bfloat16)

    hidden_ring, hidden_last = ring(shard, "z")
    outs = [product(pair) for pair in hidden_ring]
    ends = product((shard, hidden_last))
    lo = [o[:small] for o in outs]
    hi = [o[small:] for o in outs]
    terms = jnp.stack([ends[:small], *hi, ends[small:], lo[2], lo[1], lo[0]])

    def terms_for(shift):
        first = 2 * ((y + shift) % 4)
        return jnp.concatenate([pick(terms, (first + i - z) % 8) for i in (0, 1)], axis=0)

    wide = lambda a: a.astype(jnp.float32)
    half = 2 * count * rows
    two_on = terms_for(2)
    for_next, for_last = moved(two_on[:, :half], "y", 1), moved(two_on[:, half:], "y", -1)
    next_one, last_one = terms_for(1), terms_for(3)
    left = (wide(next_one[:, :half]) + wide(for_next)).astype(jnp.bfloat16)
    right = (wide(last_one[:, half:]) + wide(for_last)).astype(jnp.bfloat16)
    from_last = moved(jnp.concatenate([left, next_one[:, half:]], axis=1), "y", 1)
    from_next = moved(jnp.concatenate([last_one[:, :half], right], axis=1), "y", -1)
    summed = wide(terms_for(0)) + wide(from_last) + wide(from_next)

    summed = summed.reshape(block, 4, count, rows)
    primal = summed[:, :, 0]
    tangents = summed[:, :, 1:]
    squashed = jax.nn.sigmoid(primal)
    slope = squashed * (1.0 - squashed)
    tangent_sq = jnp.sum(tangents * tangents, axis=2)
    local_curv = jnp.sum(slope * tangent_sq, axis=(1, 2)) / (PROBES * 32 * rows)

    spread = jnp.broadcast_to(local_curv[None, None], (32, 1, block))
    everyones = lax.all_to_all(spread, ("xh", "z", "c"), 0, 0, tiled=True)
    curv = jnp.sum(everyones.reshape(2, 8, 2, block), axis=1)
    curv = curv.reshape(2, 2, 2, small).transpose(2, 0, 1, 3).reshape(4 * block)

    placed = primal.astype(jnp.bfloat16).transpose(1, 0, 2)
    placed = [
        placed[0],
        flipped(placed[1], "xh"),
        flipped(placed[2], "c"),
        flipped(placed[3], "xh", "c"),
    ]
    placed = jnp.stack(placed)
    placed = jnp.stack([pick(placed, 2 * (c ^ h) + (xh ^ t)) for t in (0, 1) for h in (0, 1)])
    placed = placed.reshape(4, 2, small, rows).transpose(1, 0, 2, 3)
    return (placed.reshape(4 * block, rows), curv)


def solution(mesh):
    def step(*arrays):
        return on_device(*arrays)

    fine = Mesh(mesh.devices.reshape(tuple(AXES.values())), tuple(AXES))
    fsdp, tp = ("xh", "z", "c"), ("xl", "y")
    step = jax.shard_map(
        step,
        mesh=fine,
        in_specs=(
            P(fsdp, tp),
            P(),
            P(fsdp, tp),
            P(fsdp, tp),
            P(fsdp, tp),
            P(None, fsdp, tp),
        ),
        out_specs=(P(tp, fsdp), P(tp)),
        check_vma=False,
    )
    return step
```

```python
import jax
import jax.numpy as jnp
from jax import lax
from jax.sharding import Mesh
from jax.sharding import PartitionSpec as P

PROBES = 2
AXES = {"xh": 2, "z": 8, "c": 2, "xl": 2, "y": 4}

epsilon = 1e-06


def moved(array, axis, shift):
    n = AXES[axis]
    return lax.ppermute(array, axis, [(i, (i + shift) % n) for i in range(n)])


def flipped(array, *axes):
    n = 2 ** len(axes)
    return lax.ppermute(array, axes, [(i, n - 1 - i) for i in range(n)])


def pick(stack, index):
    return lax.dynamic_index_in_dim(stack, index, 0, keepdims=False)


def by_index(own, other, index):
    first = index == 0
    return jnp.stack([jnp.where(first, own, other), jnp.where(first, other, own)])


def after(array, *others):
    return lax.optimization_barrier((array, *others))[0]


def ring(own, axis, gates=None):
    got, down, up = [], own, own
    for i in range(3):
        if i:
            down, up = lax.optimization_barrier((down, up, *(gates or {}).get(i, ())))[:2]
        down = moved(down, axis, 1)
        up = moved(up, axis, -1)
        got.append((down, up))
    down, up = lax.optimization_barrier((down, up))
    half = own.shape[0] // 2
    top = moved(down[:half], axis, 1)
    bottom = moved(up[half:], axis, -1)
    return got, jnp.concatenate((top, bottom), axis=0)


def on_device(tokens, norm_gain, gate_weight, up_weight, down_weight, probes):
    xh, z, c, xl, y = (lax.axis_index(a) for a in AXES)
    rows, units = gate_weight.shape
    block, width = tokens.shape
    part = units // 4
    count = 1 + PROBES

    halves = [w.reshape(rows, 4, part).transpose(1, 0, 2) for w in (gate_weight, up_weight)]
    quarters = jnp.concatenate(halves, axis=2)
    quarter = lambda a, b: pick(quarters, 2 * a + b)
    for_core = jnp.stack([quarter(xh, 1 - c), quarter(1 - xh, 1 - c)])
    from_core = flipped(for_core, "c")
    near = by_index(quarter(xh, c), from_core[0], c).reshape(2 * rows, 2 * part)
    far = by_index(quarter(1 - xh, c), from_core[1], c).reshape(2 * rows, 2 * part)
    far = flipped(far, "xh")
    near = jnp.concatenate([near, far], axis=0)

    flat = jnp.concatenate([down_weight[None], probes], axis=0).reshape(count * rows, units)
    flat = after(flat, far)
    next_xl = flipped(flat, "xl")
    next_x = flipped(flat, "xh", "xl")
    weight_ring, weight_last = ring(near, "z")
    next_xh = flipped(flat, "xh")
    spread = after(jnp.broadcast_to(tokens.T[None], (16, width, block)), from_core)
    features = lax.all_to_all(spread, ("xh", "xl", "y"), 0, 0, tiled=True)
    features = after(features, *weight_ring[0]).reshape(2, 8 * width, block)
    widened = features.astype(jnp.float32)
    inverse_rms = lax.rsqrt(jnp.mean(widened * widened, axis=1, keepdims=True) + epsilon)
    gain = norm_gain.astype(jnp.float32)[:, None]
    normed = (widened * inverse_rms * gain).astype(jnp.bfloat16)
    partner = flipped(normed, "c")
    normed = jnp.concatenate([normed[0], normed[1], partner[0], partner[1]], axis=1)
    normed = normed.reshape(2, 8, 2 * rows, 4 * block)
    normed = jnp.stack([pick(normed, xh), pick(normed, 1 - xh)], axis=1)
    normed = normed.reshape(8, 4 * rows, 4 * block)

    own_units = jnp.concatenate([flat, next_xh], axis=0)
    other_units = jnp.concatenate([next_xl, next_x], axis=0)
    own_partner, other_partner = flipped(own_units, "c"), flipped(other_units, "c")

    def summed_over(blocks):
        left = jnp.concatenate([pick(normed, (z + i) % 8) for i, _ in blocks], axis=0)
        right = jnp.concatenate([w for _, w in blocks], axis=0)
        return lax.dot_general(
            left, right, (((0,), (0,)), ((), ())), preferred_element_type=jnp.float32
        )

    sums = summed_over([(0, near)])
    for i, (down, up) in enumerate(weight_ring):
        sums += summed_over([(7 - i, down), (i + 1, up)])
    sums += summed_over([(4, weight_last)])
    gate_sum, up_sum = sums[:, :part], sums[:, part:]
    hidden = (jax.nn.silu(gate_sum) * up_sum).astype(jnp.bfloat16)

    small = block // 2
    chunks = hidden.reshape(4, 2, small, part)
    chunks = jnp.stack(
        [pick(chunks, 2 * (c ^ c_t) + xh_t) for c_t in (0, 1) for xh_t in (0, 1)]
    )
    chunks = chunks.reshape(8, small, part)
    arrived = lax.all_to_all(chunks, ("xh", "xl", "c"), 0, 0, tiled=True)
    arrived = arrived.reshape(2, 2, 2, small, part)
    arrived = jnp.moveaxis(arrived, 1, 0)
    arrived = jnp.stack([pick(arrived, xl), pick(arrived, 1 - xl)])
    shard = arrived.transpose(3, 0, 1, 2, 4).reshape(small, 2 * units)

    own_units, other_units = lax.optimization_barrier((own_units, other_units, shard))[:2]
    own_units = jnp.concatenate([own_units, own_partner], axis=0)
    other_units = jnp.concatenate([other_units, other_partner], axis=0)

    def product(blocks):
        tok = jnp.concatenate(blocks, axis=0)
        first, second = [
            lax.dot_general(t, m, (((1,), (1,)), ((), ())), preferred_element_type=jnp.float32)
            for t, m in ((tok[:, :units], own_units), (tok[:, units:], other_units))
        ]
        return (first + second).astype(jnp.bfloat16)

    hidden_ring, hidden_last = ring(shard, "z")
    outs = [product(pair) for pair in hidden_ring]
    ends = product((shard, hidden_last))
    lo = [o[:small] for o in outs]
    hi = [o[small:] for o in outs]
    terms = jnp.stack([ends[:small], *hi, ends[small:], lo[2], lo[1], lo[0]])

    def terms_for(shift):
        first = 2 * ((y + shift) % 4)
        return jnp.concatenate([pick(terms, (first + i - z) % 8) for i in (0, 1)], axis=0)

    wide = lambda a: a.astype(jnp.float32)
    half = 2 * count * rows
    two_on = terms_for(2)
    for_next, for_last = moved(two_on[:, :half], "y", 1), moved(two_on[:, half:], "y", -1)
    next_one, last_one = terms_for(1), terms_for(3)
    left = (wide(next_one[:, :half]) + wide(for_next)).astype(jnp.bfloat16)
    right = (wide(last_one[:, half:]) + wide(for_last)).astype(jnp.bfloat16)
    from_last = moved(jnp.concatenate([left, next_one[:, half:]], axis=1), "y", 1)
    from_next = moved(jnp.concatenate([last_one[:, :half], right], axis=1), "y", -1)
    summed = wide(terms_for(0)) + wide(from_last) + wide(from_next)

    summed = summed.reshape(block, 4, count, rows)
    primal = summed[:, :, 0]
    tangents = summed[:, :, 1:]
    squashed = jax.nn.sigmoid(primal)
    slope = squashed * (1.0 - squashed)
    tangent_sq = jnp.sum(tangents * tangents, axis=2)
    local_curv = jnp.sum(slope * tangent_sq, axis=(1, 2)) / (PROBES * 32 * rows)

    spread = jnp.broadcast_to(local_curv[None, None], (32, 1, block))
    everyones = lax.all_to_all(spread, ("xh", "z", "c"), 0, 0, tiled=True)
    curv = jnp.sum(everyones.reshape(2, 8, 2, block), axis=1)
    curv = curv.reshape(2, 2, 2, small).transpose(2, 0, 1, 3).reshape(4 * block)

    placed = primal.astype(jnp.bfloat16).transpose(1, 0, 2)
    placed = [
        placed[0],
        flipped(placed[1], "xh"),
        flipped(placed[2], "c"),
        flipped(placed[3], "xh", "c"),
    ]
    placed = jnp.stack(placed)
    placed = jnp.stack([pick(placed, 2 * (c ^ h) + (xh ^ t)) for t in (0, 1) for h in (0, 1)])
    placed = placed.reshape(4, 2, small, rows).transpose(1, 0, 2, 3)
    return (placed.reshape(4 * block, rows), curv)


def solution(mesh):
    def step(*arrays):
        return on_device(*arrays)

    fine = Mesh(mesh.devices.reshape(tuple(AXES.values())), tuple(AXES))
    fsdp, tp = ("xh", "z", "c"), ("xl", "y")
    step = jax.shard_map(
        step,
        mesh=fine,
        in_specs=(
            P(fsdp, tp),
            P(),
            P(fsdp, tp),
            P(fsdp, tp),
            P(fsdp, tp),
            P(None, fsdp, tp),
        ),
        out_specs=(P(tp, fsdp), P(tp)),
        check_vma=False,
    )
    return step
```

```python
import jax
import jax.numpy as jnp
from jax import lax
from jax.sharding import Mesh
from jax.sharding import PartitionSpec as P

PROBES = 2
AXES = {"xh": 2, "z": 8, "c": 2, "xl": 2, "y": 4}

epsilon = 1e-06


def moved(array, axis, shift):
    n = AXES[axis]
    return lax.ppermute(array, axis, [(i, (i + shift) % n) for i in range(n)])


def flipped(array, *axes):
    n = 2 ** len(axes)
    return lax.ppermute(array, axes, [(i, n - 1 - i) for i in range(n)])


def pick(stack, index):
    return lax.dynamic_index_in_dim(stack, index, 0, keepdims=False)


def by_index(own, other, index):
    first = index == 0
    return jnp.stack([jnp.where(first, own, other), jnp.where(first, other, own)])


def after(array, *others):
    return lax.optimization_barrier((array, *others))[0]


def ring(own, axis, gates=None):
    got, down, up = [], own, own
    for i in range(3):
        if i:
            down, up = lax.optimization_barrier((down, up, *(gates or {}).get(i, ())))[:2]
        down = moved(down, axis, 1)
        up = moved(up, axis, -1)
        got.append((down, up))
    down, up = lax.optimization_barrier((down, up))
    half = own.shape[0] // 2
    top = moved(down[:half], axis, 1)
    bottom = moved(up[half:], axis, -1)
    return got, jnp.concatenate((top, bottom), axis=0)


def on_device(tokens, norm_gain, gate_weight, up_weight, down_weight, probes):
    xh, z, c, xl, y = (lax.axis_index(a) for a in AXES)
    rows, units = gate_weight.shape
    block, width = tokens.shape
    part = units // 4
    count = 1 + PROBES

    halves = [w.reshape(rows, 4, part).transpose(1, 0, 2) for w in (gate_weight, up_weight)]
    quarters = jnp.concatenate(halves, axis=2)
    quarter = lambda a, b: pick(quarters, 2 * a + b)
    for_core = jnp.stack([quarter(xh, 1 - c), quarter(1 - xh, 1 - c)])
    from_core = flipped(for_core, "c")
    near = by_index(quarter(xh, c), from_core[0], c).reshape(2 * rows, 2 * part)
    far = by_index(quarter(1 - xh, c), from_core[1], c).reshape(2 * rows, 2 * part)
    far = flipped(far, "xh")
    near = jnp.concatenate([near, far], axis=0)

    flat = jnp.concatenate([down_weight[None], probes], axis=0).reshape(count * rows, units)
    flat = after(flat, far)
    next_xl = flipped(flat, "xl")
    next_x = flipped(flat, "xh", "xl")
    weight_ring, weight_last = ring(near, "z")
    next_xh = flipped(flat, "xh")
    spread = after(jnp.broadcast_to(tokens.T[None], (16, width, block)), from_core)
    features = lax.all_to_all(spread, ("xh", "xl", "y"), 0, 0, tiled=True)
    features = after(features, *weight_ring[0]).reshape(2, 8 * width, block)
    widened = features.astype(jnp.float32)
    inverse_rms = lax.rsqrt(jnp.mean(widened * widened, axis=1, keepdims=True) + epsilon)
    gain = norm_gain.astype(jnp.float32)[:, None]
    normed = (widened * inverse_rms * gain).astype(jnp.bfloat16)
    partner = flipped(normed, "c")
    normed = jnp.concatenate([normed[0], normed[1], partner[0], partner[1]], axis=1)
    normed = normed.reshape(2, 8, 2 * rows, 4 * block)
    normed = jnp.stack([pick(normed, xh), pick(normed, 1 - xh)], axis=1)
    normed = normed.reshape(8, 4 * rows, 4 * block)

    own_units = jnp.concatenate([flat, next_xh], axis=0)
    other_units = jnp.concatenate([next_xl, next_x], axis=0)
    own_partner, other_partner = flipped(own_units, "c"), flipped(other_units, "c")

    def summed_over(blocks):
        left = jnp.concatenate([pick(normed, (z + i) % 8) for i, _ in blocks], axis=0)
        right = jnp.concatenate([w for _, w in blocks], axis=0)
        return lax.dot_general(
            left, right, (((0,), (0,)), ((), ())), preferred_element_type=jnp.float32
        )

    sums = summed_over([(0, near)])
    for i, (down, up) in enumerate(weight_ring):
        sums += summed_over([(7 - i, down), (i + 1, up)])
    sums += summed_over([(4, weight_last)])
    gate_sum, up_sum = sums[:, :part], sums[:, part:]
    hidden = (jax.nn.silu(gate_sum) * up_sum).astype(jnp.bfloat16)

    small = block // 2
    chunks = hidden.reshape(4, 2, small, part)
    chunks = jnp.stack(
        [pick(chunks, 2 * (c ^ c_t) + xh_t) for c_t in (0, 1) for xh_t in (0, 1)]
    )
    chunks = chunks.reshape(8, small, part)
    arrived = lax.all_to_all(chunks, ("xh", "xl", "c"), 0, 0, tiled=True)
    order = [4 * a + 2 * (xl ^ d) + b for d in (0, 1) for a in (0, 1) for b in (0, 1)]
    shard = jnp.concatenate([pick(arrived, i) for i in order], axis=1)

    own_units, other_units = lax.optimization_barrier((own_units, other_units, shard))[:2]
    own_units = jnp.concatenate([own_units, own_partner], axis=0)
    other_units = jnp.concatenate([other_units, other_partner], axis=0)

    def product(blocks):
        tok = jnp.concatenate(blocks, axis=0)
        first, second = [
            lax.dot_general(t, m, (((1,), (1,)), ((), ())), preferred_element_type=jnp.float32)
            for t, m in ((tok[:, :units], own_units), (tok[:, units:], other_units))
        ]
        return (first + second).astype(jnp.bfloat16)

    hidden_ring, hidden_last = ring(shard, "z")
    outs = [product(pair) for pair in hidden_ring]
    ends = product((shard, hidden_last))
    lo = [o[:small] for o in outs]
    hi = [o[small:] for o in outs]
    terms = jnp.stack([ends[:small], *hi, ends[small:], lo[2], lo[1], lo[0]])

    def terms_for(shift):
        first = 2 * ((y + shift) % 4)
        return jnp.concatenate([pick(terms, (first + i - z) % 8) for i in (0, 1)], axis=0)

    wide = lambda a: a.astype(jnp.float32)
    half = 2 * count * rows
    two_on = terms_for(2)
    for_next, for_last = moved(two_on[:, :half], "y", 1), moved(two_on[:, half:], "y", -1)
    next_one, last_one = terms_for(1), terms_for(3)
    left = (wide(next_one[:, :half]) + wide(for_next)).astype(jnp.bfloat16)
    right = (wide(last_one[:, half:]) + wide(for_last)).astype(jnp.bfloat16)
    from_last = moved(jnp.concatenate([left, next_one[:, half:]], axis=1), "y", 1)
    from_next = moved(jnp.concatenate([last_one[:, :half], right], axis=1), "y", -1)
    summed = wide(terms_for(0)) + wide(from_last) + wide(from_next)

    summed = summed.reshape(block, 4, count, rows)
    primal = summed[:, :, 0]
    tangents = summed[:, :, 1:]
    squashed = jax.nn.sigmoid(primal)
    slope = squashed * (1.0 - squashed)
    tangent_sq = jnp.sum(tangents * tangents, axis=2)
    local_curv = jnp.sum(slope * tangent_sq, axis=(1, 2)) / (PROBES * 32 * rows)

    spread = jnp.broadcast_to(local_curv[None, None], (32, 1, block))
    everyones = lax.all_to_all(spread, ("xh", "z", "c"), 0, 0, tiled=True)
    curv = jnp.sum(everyones.reshape(2, 8, 2, block), axis=1)
    curv = curv.reshape(2, 2, 2, small).transpose(2, 0, 1, 3).reshape(4 * block)

    placed = primal.astype(jnp.bfloat16).transpose(1, 0, 2)
    placed = [
        placed[0],
        flipped(placed[1], "xh"),
        flipped(placed[2], "c"),
        flipped(placed[3], "xh", "c"),
    ]
    placed = jnp.stack(placed)
    placed = jnp.stack([pick(placed, 2 * (c ^ h) + (xh ^ t)) for t in (0, 1) for h in (0, 1)])
    placed = placed.reshape(4, 2, small, rows).transpose(1, 0, 2, 3)
    return (placed.reshape(4 * block, rows), curv)


def solution(mesh):
    def step(*arrays):
        return on_device(*arrays)

    fine = Mesh(mesh.devices.reshape(tuple(AXES.values())), tuple(AXES))
    fsdp, tp = ("xh", "z", "c"), ("xl", "y")
    step = jax.shard_map(
        step,
        mesh=fine,
        in_specs=(
            P(fsdp, tp),
            P(),
            P(fsdp, tp),
            P(fsdp, tp),
            P(fsdp, tp),
            P(None, fsdp, tp),
        ),
        out_specs=(P(tp, fsdp), P(tp)),
        check_vma=False,
    )
    return step
```
